32 devices in a mesh: seq: 8 (over y, x, core), grp: 4 (over z).
Axes of the slice: x: 2, y: 2, z: 4, core: 2. Of those that a mesh axis runs over, the one named last changes fastest.
Arguments:
- queries: bfloat16 [4096, 2048], P(('seq', 'grp')), may hold values from -8 to 8
- keys: bfloat16 [4096, 128], P(('seq', 'grp')), may hold values from -8 to 8
- values: bfloat16 [4096, 128], P(('seq', 'grp')), may hold values from -6 to 6
- cotangent: bfloat16 [4096, 2048], P(('seq', 'grp')), may hold values from -6 to 6
- doc_lengths: int32 [8], replicated, may hold values from 1 to 1024, 4096 in all
Outputs:
- attn_out: bfloat16 [4096, 2048], P(('seq', 'grp'))
- grad_queries: bfloat16 [4096, 2048], P(('seq', 'grp'))
- grad_keys: bfloat16 [4096, 128], P(('seq', 'grp'))
- grad_values: bfloat16 [4096, 128], P(('seq', 'grp'))
The draws below stay inside these ranges and needn't reach their ends.
Inputs may be any that keep to these rules, and one draw needn't show every extreme that they name: `doc_lengths`: the lengths sum to 4096, and one of them is exactly 1024.
All inputs are finite; a program needn't handle non-finite values.
Results may differ from the reference program's by a relative error of at most 0.023.
Values may be sent and summed in bfloat16 or wider, within the bound.
A program may use at most 64 MiB of HBM per device.

```python
import math
import jax
import jax.numpy as jnp
import numpy as np
from jax import lax

DH = 128
HEADS = 16
TOK_DEV = 128
REACH = 8
DOC_MOST = 1024
TOKENS = 4096
DOCS = 8


def draw_keys(key, part):
    result = jnp.clip(jax.random.normal(jax.random.fold_in(key, 11), (TOKENS, DH), jnp.float32), -8.0, 8.0)
    return result.astype(jnp.bfloat16)


def draw_queries(key, part):
    result = jnp.clip(jax.random.normal(jax.random.fold_in(key, 23), (TOKENS, HEADS * DH), jnp.float32), -8.0, 8.0)
    return result.astype(jnp.bfloat16)


def level_of(key, shape, cuts, smallest, largest):
    loudness, own = 1.0, jax.random.fold_in(key, 6)
    for dim, blocks in cuts:
        steps = jnp.exp(jax.random.uniform(jax.random.fold_in(own, dim), (blocks,), jnp.float32, smallest / len(cuts), largest / len(cuts)))
        loudness = loudness * jnp.repeat(steps, shape[dim] // blocks).reshape([-1 if axis == dim else 1 for axis in range(len(shape))])
    return loudness


def profile(number_of, total, most, skew):
    weights = [(1 << 20) // math.isqrt(grade ** skew) + 1 for grade in range(2, number_of + 1)]
    surplus, holding = total - most - (number_of - 1), [1] * (number_of - 1)
    while surplus > 0:
        movable = [i for i in range(number_of - 1) if holding[i] < most]
        pool, remaining = sum([weights[i] for i in movable]), surplus
        for i in movable:
            addition = min(most - holding[i], max(1, remaining * weights[i] // pool), surplus)
            holding[i] = holding[i] + addition
            surplus = surplus - addition
    return np.array([most] + holding)


def uneven_parts(key, amount, total, limit, skew):
    if amount == 2:
        one = jax.random.randint(key, (), max(1, total - limit), min(limit, total - 1) + 1)
        return jnp.stack([one, total - one])
    tallies = jnp.asarray(profile(amount, total, limit, skew), jnp.int32)
    twos = (amount - 1) // 2
    donor, receiver = tallies[1:1 + 2 * twos:2], tallies[2:2 + 2 * twos:2]
    slack = jnp.minimum(donor - 1, limit - receiver)
    moved = jax.random.randint(jax.random.fold_in(key, 1), (twos,), 0, 1 << 20) % (slack + 1)
    tallies = tallies.at[1:1 + 2 * twos:2].set(donor - moved).at[2:2 + 2 * twos:2].set(receiver + moved)
    return tallies[jax.random.permutation(jax.random.fold_in(key, 2), amount)]


def centred(own_key, dims, width, most, pieces=(), kind=jnp.bfloat16):
    factor_of = level_of(own_key, dims, pieces, -0.22, 0.18) if pieces else 1.0
    values = jax.random.normal(own_key, dims, jnp.float32) * width * factor_of
    return jnp.minimum(jnp.maximum(values, -most), most).astype(kind)


def setup_inputs(seed: int = 0) -> dict:
    key_list = jax.random.split(jax.random.key(seed), 6)
    queries = draw_queries(jax.random.fold_in(key_list[5], 71), 0)
    keys = draw_keys(jax.random.fold_in(key_list[5], 71), 0)
    values = centred(key_list[2], (TOKENS, DH), 1.0, 6.0, ((0, 32),))
    cotangent = centred(key_list[3], (TOKENS, HEADS * DH), 1.0, 6.0, ((0, 32),))
    doc_lengths = uneven_parts(key_list[4], DOCS, TOKENS, DOC_MOST, 2).astype(jnp.int32)
    return dict(queries=queries, keys=keys, values=values, cotangent=cotangent, doc_lengths=doc_lengths)


def doc_number(positions, doc_ends):
    return jnp.sum((doc_ends[None, :] <= positions[:, None]).astype(jnp.int32), axis=1)


def reference(queries, keys, values, cotangent, doc_lengths):
    block_rows = TOK_DEV
    span_rows = (REACH + 1) * block_rows
    scaling = DH ** -0.5
    doc_ends = jnp.cumsum(doc_lengths).astype(jnp.int32)
    padding = jnp.zeros((REACH * block_rows, DH), keys.dtype)
    keys_pad = jnp.concatenate([padding, keys], axis=0)
    values_pad = jnp.concatenate([padding, values], axis=0)

    def one_block(grad_store, block_index):
        offset = (block_index * block_rows).astype(jnp.int32)
        query_part = lax.dynamic_slice_in_dim(queries, offset, block_rows, 0).reshape(block_rows, HEADS, DH).astype(jnp.float32)
        upstream = lax.dynamic_slice_in_dim(cotangent, offset, block_rows, 0).reshape(block_rows, HEADS, DH).astype(jnp.float32)
        keys_win = lax.dynamic_slice_in_dim(keys_pad, offset, span_rows, 0).astype(jnp.float32)
        values_win = lax.dynamic_slice_in_dim(values_pad, offset, span_rows, 0).astype(jnp.float32)
        query_pos = offset + jnp.arange(block_rows, dtype=jnp.int32)
        key_pos = offset - REACH * block_rows + jnp.arange(span_rows, dtype=jnp.int32)
        allowed = (key_pos[None, :] >= 0) & (key_pos[None, :] <= query_pos[:, None])
        allowed = allowed & (doc_number(key_pos, doc_ends)[None, :] == doc_number(query_pos, doc_ends)[:, None])
        scores = jnp.einsum("thd,kd->thk", query_part, keys_win) * scaling
        scores = jnp.where(allowed[:, None, :], scores, -jnp.inf)
        row_peak = jnp.max(scores, axis=2, keepdims=True)
        exponent = jnp.exp(scores - row_peak)
        weights = exponent / jnp.sum(exponent, axis=2, keepdims=True)
        weights_low = lax.optimization_barrier(weights.astype(jnp.bfloat16)).astype(jnp.float32)
        attended = jnp.einsum("thk,kd->thd", weights_low, values_win)
        attended_low = lax.optimization_barrier(attended.astype(jnp.bfloat16))
        row_dot = jnp.sum(upstream * attended_low.astype(jnp.float32), axis=2, keepdims=True)
        grad_weights = jnp.einsum("thd,kd->thk", upstream, values_win)
        grad_scores = lax.optimization_barrier((weights * (grad_weights - row_dot)).astype(jnp.bfloat16)).astype(jnp.float32)
        grad_part = (jnp.einsum("thk,kd->thd", grad_scores, keys_win) * scaling).astype(jnp.bfloat16)
        grad_keys = jnp.einsum("thk,thd->kd", grad_scores, query_part) * scaling
        grad_values = jnp.einsum("thk,thd->kd", weights_low, upstream)
        current = lax.dynamic_slice_in_dim(grad_store, offset, span_rows, 0)
        grad_store = lax.dynamic_update_slice_in_dim(grad_store, current + jnp.concatenate([grad_keys, grad_values], axis=1), offset, 0)
        return grad_store, (attended_low.reshape(block_rows, HEADS * DH), grad_part.reshape(block_rows, HEADS * DH))

    store_init = jnp.zeros((TOKENS + REACH * block_rows, 2 * DH), jnp.float32)
    grad_store, (attended_all, grad_query_all) = lax.scan(one_block, store_init, jnp.arange(TOKENS // block_rows, dtype=jnp.int32))
    attn_out = attended_all.reshape(TOKENS, HEADS * DH)
    grad_queries = grad_query_all.reshape(TOKENS, HEADS * DH)
    owned = grad_store[REACH * block_rows:]
    return attn_out, grad_queries, owned[:, :DH].astype(jnp.bfloat16), owned[:, DH:].astype(jnp.bfloat16)
```

```python
import functools

import jax
import jax.numpy as jnp
from jax import lax
from jax.experimental import pallas as pl
from jax.experimental.pallas import tpu as pltpu
from jax.sharding import PartitionSpec as P

REACH = 8
HALF = REACH // 2
GROUP_HEADS = 4
MASKED = -1e30
LOG2E = 1.4426950408889634
PLACES = (0, 1, 3, 4, 2, 5, 6, 7, 8)


def kernel(
    count,
    members,
    lengths_hbm,
    queries_hbm,
    keys_hbm,
    values_hbm,
    cotangent_hbm,
    out_ref,
    grad_queries_ref,
    grad_keys_ref,
    grad_values_ref,
    window,
    queries_t,
    cotangent_t,
    keys_t,
    values_t,
    probs,
    grad_probs,
    peaks,
    sums,
    dots,
    row_dots,
    weights_low,
    grad_scores,
    grad_window,
    grad_send,
    grad_far,
    grad_near,
    send_sems,
    recv_sems,
    grad_send_sems,
    grad_recv_sems,
    lengths_ref,
    stacked,
    keys_ref,
    values_ref,
    load_sems,
):
    rows, head_size = keys_ref.shape
    head_count = stacked.shape[0] // rows
    heads = min(head_count, GROUP_HEADS)
    width = heads * rows
    groups = head_count // heads
    scaling = head_size ** (-0.5)
    me = lax.axis_index("seq") * members + lax.axis_index("grp")

    def place(index):
        return (lax.div(index, members), lax.rem(index, members))

    def key_copy(distance, half):
        source = (keys_ref, values_ref)[half]
        target = me + distance
        if distance > HALF:
            source = window.at[distance - HALF, half]
            target = me + HALF
        return pltpu.make_async_remote_copy(
            src_ref=source,
            dst_ref=window.at[distance, half],
            send_sem=send_sems.at[distance, half],
            recv_sem=recv_sems.at[distance, half],
            device_id=place(target),
            device_id_type=pl.DeviceIdType.MESH,
        )

    def grad_copy(distance):
        if distance > HALF:
            target, slot = me - HALF, grad_far.at[distance - HALF]
        else:
            target, slot = me - distance, grad_near.at[distance]
        return pltpu.make_async_remote_copy(
            src_ref=grad_send.at[distance],
            dst_ref=slot,
            send_sem=grad_send_sems.at[distance],
            recv_sem=grad_recv_sems.at[distance],
            device_id=place(target),
            device_id_type=pl.DeviceIdType.MESH,
        )

    pairs = [
        (keys_hbm, keys_ref),
        (values_hbm, values_ref),
        (lengths_hbm, lengths_ref),
    ]
    for half, source in enumerate((queries_hbm, cotangent_hbm)):
        for head in range(head_count):
            pairs.append(
                (
                    source.at[:, head * head_size : (head + 1) * head_size],
                    stacked.at[
                        head * rows : (head + 1) * rows,
                        half * head_size : (half + 1) * head_size,
                    ],
                )
            )
    loads = [
        pltpu.make_async_copy(source, target, load_sems.at[index])
        for index, (source, target) in enumerate(pairs)
    ]
    for load in loads:
        load.start()

    barrier = pltpu.get_barrier_semaphore()
    for distance in range(1, HALF + 1):
        for there in (me + distance, me - distance):

            @pl.when((there >= 0) & (there < count))
            def _():
                pl.semaphore_signal(
                    barrier, inc=1, device_id=place(there), device_id_type=pl.DeviceIdType.MESH
                )

    for distance in range(1, REACH + 1):

        @pl.when(me < distance)
        def _():
            window[distance] = jnp.zeros_like(window.at[distance])

    for distance in range(1, HALF + 1):

        @pl.when(me + distance >= count)
        def _():
            grad_near[distance] = jnp.zeros_like(grad_near.at[distance])

        @pl.when((me + HALF >= count) | (me < distance))
        def _():
            grad_far[distance] = jnp.zeros_like(grad_far.at[distance])

    for load in loads[:3]:
        load.wait()
    query_pos = me * rows + lax.broadcasted_iota(jnp.int32, (1, rows), 1)

    def one_doc(doc, state):
        end, start = state
        end = end + lengths_ref[doc]
        return end, jnp.where(query_pos >= end, end, start)

    _, doc_start = lax.fori_loop(
        0, lengths_ref.shape[0], one_doc, (jnp.int32(0), jnp.zeros((1, rows), jnp.int32))
    )

    for load in loads[3:]:
        load.wait()
    for head in range(head_count):
        columns = slice(head * rows, (head + 1) * rows)
        queries_t[:, columns] = stacked[columns, 0:head_size].T
        cotangent_t[:, columns] = stacked[columns, head_size:].T

    def block_rows(distance):
        return slice(PLACES[distance] * rows, (PLACES[distance] + 1) * rows)

    def block_of(distance):
        if distance == 0:
            return keys_ref[...], values_ref[...]
        return window[distance, 0], window[distance, 1]

    def score_block(distance):
        keys, values = block_of(distance)
        span = block_rows(distance)
        keys_t[:, span] = keys.T
        values_t[:, span] = values.T
        key_pos = (me - distance) * rows + lax.broadcasted_iota(jnp.int32, (rows, rows), 0)
        allowed = key_pos >= doc_start
        if distance == 0:
            allowed = allowed & (key_pos <= query_pos)
        bias = jnp.where(allowed, 0.0, MASKED).astype(jnp.float32)
        bias = jnp.concatenate([bias] * heads, axis=1)

        def folded(part, op):
            return op(part.reshape(rows // 8, 8, width), axis=0)

        for group in range(groups):
            columns = slice(group * width, (group + 1) * width)
            scores = jnp.dot(keys, queries_t[:, columns], preferred_element_type=jnp.float32)
            scores = scores * (scaling * LOG2E) + bias
            peak = folded(scores, jnp.max)
            prob = jnp.exp2(scores.reshape(rows // 8, 8, width) - peak[None]).reshape(rows, width)
            grad_prob = jnp.dot(values, cotangent_t[:, columns], preferred_element_type=jnp.float32)
            probs[span, columns] = prob
            grad_probs[span, columns] = grad_prob
            peaks[distance, :, columns] = peak
            sums[distance, :, columns] = folded(prob, jnp.sum)
            dots[distance, :, columns] = folded(prob * grad_prob, jnp.sum)

    score_block(0)
    pl.semaphore_wait(barrier, jnp.minimum(me, HALF) + jnp.minimum(count - 1 - me, HALF))

    for distance in (4, 3, 2, 1):

        @pl.when(me + distance < count)
        def _():
            for half in range(2):
                key_copy(distance, half).start()

    for distance in (4, 1, 2, 3):

        @pl.when(me >= distance)
        def _():
            for half in range(2):
                key_copy(distance, half).wait_recv()

        @pl.when((me >= distance) & (me + HALF < count))
        def _():
            for half in range(2):
                key_copy(distance + HALF, half).start()

        score_block(distance)
    for distance in (8, 5, 6, 7):

        @pl.when(me >= distance)
        def _():
            for half in range(2):
                key_copy(distance, half).wait_recv()

        score_block(distance)

    for group in range(groups):
        columns = slice(group * width, (group + 1) * width)
        top = peaks[0, :, columns]
        for distance in range(1, REACH + 1):
            top = jnp.maximum(top, peaks[distance, :, columns])
        top = jnp.max(top, axis=0, keepdims=True)
        total = jnp.zeros((8, width), jnp.float32)
        dot = total
        for distance in range(REACH + 1):
            factor = jnp.exp2(peaks[distance, :, columns] - top)
            peaks[distance, :, columns] = factor
            total = total + factor * sums[distance, :, columns]
            dot = dot + factor * dots[distance, :, columns]
        inverse = 1.0 / jnp.sum(total, axis=0, keepdims=True)
        row_dots[:, columns] = jnp.broadcast_to(
            jnp.sum(dot, axis=0, keepdims=True) * inverse, (8, width)
        )
        for distance in range(REACH + 1):
            peaks[distance, :, columns] = peaks[distance, :, columns] * inverse

    def grad_blocks(distances):
        size = len(distances) * rows
        first = PLACES[distances[0]]
        span = slice(first * rows, first * rows + size)
        tiles = (rows // 8, 8, width)
        for group in range(groups):
            columns = slice(group * width, (group + 1) * width)
            row_dot = row_dots[:, columns]
            for distance in distances:
                block = block_rows(distance)
                weights = probs[block, columns].reshape(tiles) * peaks[distance, :, columns][None]
                weights_low[block, columns] = weights.reshape(rows, width).astype(jnp.bfloat16)
                grads = weights * (grad_probs[block, columns].reshape(tiles) - row_dot[None])
                grad_scores[block, columns] = grads.reshape(rows, width).astype(jnp.bfloat16)
        for half, left in enumerate((grad_scores, weights_low)):
            both = jnp.dot(left[span, :], stacked[...], preferred_element_type=jnp.float32)
            grad_window[half, span, :] = both[:, half * head_size : (half + 1) * head_size]

    grad_blocks((5, 6, 7, 8))
    for distance in range(REACH, HALF, -1):
        block = block_rows(distance)

        @pl.when(me >= distance)
        def _():
            for half in range(2):
                grad_send[distance, half] = grad_window[half, block, :].astype(jnp.bfloat16)
            grad_copy(distance).start()

    def send_near(distance):
        block = block_rows(distance)

        @pl.when((me >= distance) & (me + HALF < count))
        def _():
            grad_copy(distance + HALF).wait_recv()

        @pl.when(me >= distance)
        def _():
            for half in range(2):
                grad_send[distance, half] = (
                    grad_window[half, block, :] + grad_far[distance, half].astype(jnp.float32)
                ).astype(jnp.bfloat16)
            grad_copy(distance).start()

    for distances in ((2, 3), (1, 4)):
        grad_blocks(distances)
        for distance in reversed(distances):
            send_near(distance)

    grad_blocks((0,))
    for group in range(groups):
        columns = slice(group * width, (group + 1) * width)
        out_part = jnp.dot(
            values_t[...], weights_low[:, columns], preferred_element_type=jnp.float32
        ).astype(jnp.bfloat16)
        grad_part = jnp.dot(
            keys_t[...], grad_scores[:, columns], preferred_element_type=jnp.float32
        )
        grad_part = (grad_part * scaling).astype(jnp.bfloat16)
        for head in range(heads):
            local = slice(head * rows, (head + 1) * rows)
            first = (group * heads + head) * head_size
            out_ref[:, first : first + head_size] = out_part[:, local].T
            grad_queries_ref[:, first : first + head_size] = grad_part[:, local].T

    for distance in range(1, HALF + 1):

        @pl.when(me + distance < count)
        def _():
            grad_copy(distance).wait_recv()

    owned = []
    for half in range(2):
        part = grad_window[half, 0:rows, :]
        for distance in range(1, HALF + 1):
            part = part + grad_near[distance, half].astype(jnp.float32)
        owned.append(part)
    grad_keys_ref[...] = (owned[0] * scaling).astype(jnp.bfloat16)
    grad_values_ref[...] = owned[1].astype(jnp.bfloat16)

    for distance in range(1, REACH + 1):
        reachable = me + distance < count
        if distance > HALF:
            reachable = (me >= distance - HALF) & (me + HALF < count)

        @pl.when(reachable)
        def _():
            for half in range(2):
                key_copy(distance, half).wait_send()

        @pl.when(me >= distance)
        def _():
            grad_copy(distance).wait_send()


def settle(*refs):
    half = len(refs) // 2
    for source, target in zip(refs[:half], refs[half:]):
        target[...] = source[...]


def per_device(queries, keys, values, cotangent, doc_lengths):
    rows, head_size = keys.shape
    head_count = queries.shape[1] // head_size
    members = lax.axis_size("grp")
    count = lax.axis_size("seq") * members
    tall = (REACH + 1) * rows
    wide = head_count * rows
    vmem = pl.BlockSpec(memory_space=pltpu.VMEM)
    far = pl.BlockSpec(memory_space=pltpu.HBM)
    low, full = jnp.bfloat16, jnp.float32
    results = pl.pallas_call(
        functools.partial(kernel, count, members),
        out_shape=(
            jax.ShapeDtypeStruct(queries.shape, low),
            jax.ShapeDtypeStruct(queries.shape, low),
            jax.ShapeDtypeStruct(keys.shape, low),
            jax.ShapeDtypeStruct(keys.shape, low),
        ),
        in_specs=[far] * 5,
        out_specs=(vmem,) * 4,
        scratch_shapes=[
            pltpu.VMEM((REACH + 1, 2, rows, head_size), low),
            pltpu.VMEM((head_size, wide), low),
            pltpu.VMEM((head_size, wide), low),
            pltpu.VMEM((head_size, tall), low),
            pltpu.VMEM((head_size, tall), low),
            pltpu.VMEM((tall, wide), full),
            pltpu.VMEM((tall, wide), full),
            pltpu.VMEM((REACH + 1, 8, wide), full),
            pltpu.VMEM((REACH + 1, 8, wide), full),
            pltpu.VMEM((REACH + 1, 8, wide), full),
            pltpu.VMEM((8, wide), full),
            pltpu.VMEM((tall, wide), low),
            pltpu.VMEM((tall, wide), low),
            pltpu.VMEM((2, tall, head_size), full),
            pltpu.VMEM((REACH + 1, 2, rows, head_size), low),
            pltpu.VMEM((HALF + 1, 2, rows, head_size), low),
            pltpu.VMEM((HALF + 1, 2, rows, head_size), low),
            pltpu.SemaphoreType.DMA((REACH + 1, 2)),
            pltpu.SemaphoreType.DMA((REACH + 1, 2)),
            pltpu.SemaphoreType.DMA((REACH + 1,)),
            pltpu.SemaphoreType.DMA((REACH + 1,)),
            pltpu.SMEM(doc_lengths.shape, jnp.int32),
            pltpu.VMEM((wide, 2 * head_size), low),
            pltpu.VMEM(keys.shape, low),
            pltpu.VMEM(keys.shape, low),
            pltpu.SemaphoreType.DMA((3 + 2 * head_count,)),
        ],
        compiler_params=pltpu.CompilerParams(
            collective_id=0, has_side_effects=True, vmem_limit_bytes=60 * 1024 * 1024
        ),
        name="attention",
    )(doc_lengths, queries, keys, values, cotangent)
    return pl.pallas_call(
        settle,
        out_shape=tuple(jax.ShapeDtypeStruct(result.shape, low) for result in results),
        in_specs=[vmem] * 4,
        out_specs=(vmem,) * 4,
        compiler_params=pltpu.CompilerParams(vmem_limit_bytes=60 * 1024 * 1024),
        name="settle",
    )(*results)


def solution(mesh):
    rows = P(("seq", "grp"), None)
    return jax.shard_map(
        per_device,
        mesh=mesh,
        in_specs=(rows, rows, rows, rows, P()),
        out_specs=(rows, rows, rows, rows),
        check_vma=False,
    )
```

```python
import functools

import jax
import jax.numpy as jnp
from jax import lax
from jax.experimental import pallas as pl
from jax.experimental.pallas import tpu as pltpu
from jax.sharding import PartitionSpec as P

REACH = 8
HALF = REACH // 2
GROUP_HEADS = 4
MASKED = -1e30
LOG2E = 1.4426950408889634
PLACES = (0, 1, 3, 4, 2, 5, 6, 7, 8)


def kernel(
    count,
    members,
    lengths_hbm,
    queries_hbm,
    keys_hbm,
    values_hbm,
    cotangent_hbm,
    out_ref,
    grad_queries_ref,
    grad_keys_ref,
    grad_values_ref,
    window,
    queries_t,
    cotangent_t,
    keys_t,
    values_t,
    probs,
    grad_probs,
    peaks,
    sums,
    dots,
    row_dots,
    weights_low,
    grad_scores,
    grad_window,
    grad_send,
    grad_far,
    grad_near,
    send_sems,
    recv_sems,
    grad_send_sems,
    grad_recv_sems,
    lengths_ref,
    stacked,
    keys_ref,
    values_ref,
    load_sems,
):
    rows, head_size = keys_ref.shape
    head_count = stacked.shape[0] // rows
    heads = min(head_count, GROUP_HEADS)
    width = heads * rows
    groups = head_count // heads
    scaling = head_size ** (-0.5)
    me = lax.axis_index("seq") * members + lax.axis_index("grp")

    def place(index):
        return (lax.div(index, members), lax.rem(index, members))

    member = lax.axis_index("grp")
    paired = members == HALF

    def key_copy(distance, half, step=None):
        if step is not None:
            source, slot, sender = window.at[distance, half], distance + step, 0
        elif distance > HALF:
            source, slot, sender = window.at[distance - HALF, half], distance, distance
            step = HALF
        else:
            source, slot, sender = (keys_ref, values_ref)[half], distance, distance
            step = distance
        return pltpu.make_async_remote_copy(
            src_ref=source,
            dst_ref=window.at[slot, half],
            send_sem=send_sems.at[sender, half],
            recv_sem=recv_sems.at[slot, half],
            device_id=place(me + step),
            device_id_type=pl.DeviceIdType.MESH,
        )

    def direct(distance, sender):
        within = (sender >= 0) & (sender + distance < count)
        if paired and distance == 1:
            within = within & (lax.rem(sender + members, members) <= members - 2)
        if paired and distance == HALF - 1:
            within = within & (lax.rem(sender + members, members) >= 1)
        return within

    turns = ()
    if paired:
        middle = HALF // 2
        turns = (
            ((member == middle - 1) & (me >= middle), middle, -1),
            (member == middle, middle, 1),
        )

    def pass_on(distance):
        for fits, slot, step in turns:
            if slot == distance:

                @pl.when(fits)
                def _():
                    for half in range(2):
                        key_copy(distance, half, step).start()

        @pl.when((me >= distance) & (me + HALF < count))
        def _():
            for half in range(2):
                key_copy(distance + HALF, half).start()

    def grad_copy(distance):
        if distance > HALF:
            target, slot = me - HALF, grad_far.at[distance - HALF]
        else:
            target, slot = me - distance, grad_near.at[distance]
        return pltpu.make_async_remote_copy(
            src_ref=grad_send.at[distance],
            dst_ref=slot,
            send_sem=grad_send_sems.at[distance],
            recv_sem=grad_recv_sems.at[distance],
            device_id=place(target),
            device_id_type=pl.DeviceIdType.MESH,
        )

    pairs = [
        (keys_hbm, keys_ref),
        (values_hbm, values_ref),
        (lengths_hbm, lengths_ref),
    ]
    for half, source in enumerate((queries_hbm, cotangent_hbm)):
        for head in range(head_count):
            pairs.append(
                (
                    source.at[:, head * head_size : (head + 1) * head_size],
                    stacked.at[
                        head * rows : (head + 1) * rows,
                        half * head_size : (half + 1) * head_size,
                    ],
                )
            )
    loads = [
        pltpu.make_async_copy(source, target, load_sems.at[index])
        for index, (source, target) in enumerate(pairs)
    ]
    for load in loads:
        load.start()

    barrier = pltpu.get_barrier_semaphore()
    greeted = jnp.int32(0)
    for distance in range(HALF, 0, -1):
        for fits, there in (
            (direct(distance, me), me + distance),
            (direct(distance, me - distance), me - distance),
        ):
            greeted = greeted + fits.astype(jnp.int32)

            @pl.when(fits)
            def _():
                pl.semaphore_signal(
                    barrier, inc=1, device_id=place(there), device_id_type=pl.DeviceIdType.MESH
                )

    for distance in range(1, REACH + 1):

        @pl.when(me < distance)
        def _():
            window[distance] = jnp.zeros_like(window.at[distance])

    for distance in range(1, HALF + 1):

        @pl.when(me + distance >= count)
        def _():
            grad_near[distance] = jnp.zeros_like(grad_near.at[distance])

        @pl.when((me + HALF >= count) | (me < distance))
        def _():
            grad_far[distance] = jnp.zeros_like(grad_far.at[distance])

    for load in loads[:3]:
        load.wait()
    query_pos = me * rows + lax.broadcasted_iota(jnp.int32, (1, rows), 1)

    def one_doc(doc, state):
        end, start = state
        end = end + lengths_ref[doc]
        return end, jnp.where(query_pos >= end, end, start)

    _, doc_start = lax.fori_loop(
        0, lengths_ref.shape[0], one_doc, (jnp.int32(0), jnp.zeros((1, rows), jnp.int32))
    )

    for load in loads[3:]:
        load.wait()
    for head in range(head_count):
        columns = slice(head * rows, (head + 1) * rows)
        queries_t[:, columns] = stacked[columns, 0:head_size].T
        cotangent_t[:, columns] = stacked[columns, head_size:].T

    def block_rows(distance):
        return slice(PLACES[distance] * rows, (PLACES[distance] + 1) * rows)

    def block_of(distance):
        if distance == 0:
            return keys_ref[...], values_ref[...]
        return window[distance, 0], window[distance, 1]

    def score_block(distance):
        keys, values = block_of(distance)
        span = block_rows(distance)
        keys_t[:, span] = keys.T
        values_t[:, span] = values.T
        key_pos = (me - distance) * rows + lax.broadcasted_iota(jnp.int32, (rows, rows), 0)
        allowed = key_pos >= doc_start
        if distance == 0:
            allowed = allowed & (key_pos <= query_pos)
        bias = jnp.where(allowed, 0.0, MASKED).astype(jnp.float32)
        bias = jnp.concatenate([bias] * heads, axis=1)

        def folded(part, op):
            return op(part.reshape(rows // 8, 8, width), axis=0)

        for group in range(groups):
            columns = slice(group * width, (group + 1) * width)
            scores = jnp.dot(keys, queries_t[:, columns], preferred_element_type=jnp.float32)
            scores = scores * (scaling * LOG2E) + bias
            peak = folded(scores, jnp.max)
            prob = jnp.exp2(scores.reshape(rows // 8, 8, width) - peak[None]).reshape(rows, width)
            grad_prob = jnp.dot(values, cotangent_t[:, columns], preferred_element_type=jnp.float32)
            probs[span, columns] = prob
            grad_probs[span, columns] = grad_prob
            peaks[distance, :, columns] = peak
            sums[distance, :, columns] = folded(prob, jnp.sum)
            dots[distance, :, columns] = folded(prob * grad_prob, jnp.sum)

    score_block(0)
    pl.semaphore_wait(barrier, greeted)
    for distance in (4, 2, 1, 3):

        @pl.when(direct(distance, me))
        def _():
            for half in range(2):
                key_copy(distance, half).start()

    for distance in (4, 2, 1, 3, 8, 6, 5, 7):

        @pl.when(me >= distance)
        def _():
            for half in range(2):
                key_copy(distance, half).wait_recv()

        if distance <= HALF:
            pass_on(distance)
        score_block(distance)

    for group in range(groups):
        columns = slice(group * width, (group + 1) * width)
        top = peaks[0, :, columns]
        for distance in range(1, REACH + 1):
            top = jnp.maximum(top, peaks[distance, :, columns])
        top = jnp.max(top, axis=0, keepdims=True)
        total = jnp.zeros((8, width), jnp.float32)
        dot = total
        for distance in range(REACH + 1):
            factor = jnp.exp2(peaks[distance, :, columns] - top)
            peaks[distance, :, columns] = factor
            total = total + factor * sums[distance, :, columns]
            dot = dot + factor * dots[distance, :, columns]
        inverse = 1.0 / jnp.sum(total, axis=0, keepdims=True)
        row_dots[:, columns] = jnp.broadcast_to(
            jnp.sum(dot, axis=0, keepdims=True) * inverse, (8, width)
        )
        for distance in range(REACH + 1):
            peaks[distance, :, columns] = peaks[distance, :, columns] * inverse

    def grad_blocks(distances):
        size = len(distances) * rows
        first = PLACES[distances[0]]
        span = slice(first * rows, first * rows + size)
        tiles = (rows // 8, 8, width)
        for group in range(groups):
            columns = slice(group * width, (group + 1) * width)
            row_dot = row_dots[:, columns]
            for distance in distances:
                block = block_rows(distance)
                weights = probs[block, columns].reshape(tiles) * peaks[distance, :, columns][None]
                weights_low[block, columns] = weights.reshape(rows, width).astype(jnp.bfloat16)
                grads = weights * (grad_probs[block, columns].reshape(tiles) - row_dot[None])
                grad_scores[block, columns] = grads.reshape(rows, width).astype(jnp.bfloat16)
        for half, left in enumerate((grad_scores, weights_low)):
            both = jnp.dot(left[span, :], stacked[...], preferred_element_type=jnp.float32)
            grad_window[half, span, :] = both[:, half * head_size : (half + 1) * head_size]

    grad_blocks((5, 6, 7, 8))
    for distance in range(REACH, HALF, -1):
        block = block_rows(distance)

        @pl.when(me >= distance)
        def _():
            for half in range(2):
                grad_send[distance, half] = grad_window[half, block, :].astype(jnp.bfloat16)
            grad_copy(distance).start()

    def send_near(distance):
        block = block_rows(distance)

        @pl.when((me >= distance) & (me + HALF < count))
        def _():
            grad_copy(distance + HALF).wait_recv()

        @pl.when(me >= distance)
        def _():
            for half in range(2):
                grad_send[distance, half] = (
                    grad_window[half, block, :] + grad_far[distance, half].astype(jnp.float32)
                ).astype(jnp.bfloat16)
            grad_copy(distance).start()

    for distances in ((2, 3), (1, 4)):
        grad_blocks(distances)
        for distance in reversed(distances):
            send_near(distance)

    grad_blocks((0,))
    for group in range(groups):
        columns = slice(group * width, (group + 1) * width)
        out_part = jnp.dot(
            values_t[...], weights_low[:, columns], preferred_element_type=jnp.float32
        ).astype(jnp.bfloat16)
        grad_part = jnp.dot(
            keys_t[...], grad_scores[:, columns], preferred_element_type=jnp.float32
        )
        grad_part = (grad_part * scaling).astype(jnp.bfloat16)
        for head in range(heads):
            local = slice(head * rows, (head + 1) * rows)
            first = (group * heads + head) * head_size
            out_ref[:, first : first + head_size] = out_part[:, local].T
            grad_queries_ref[:, first : first + head_size] = grad_part[:, local].T

    for distance in range(1, HALF + 1):

        @pl.when(me + distance < count)
        def _():
            grad_copy(distance).wait_recv()

    owned = []
    for half in range(2):
        part = grad_window[half, 0:rows, :]
        for distance in range(1, HALF + 1):
            part = part + grad_near[distance, half].astype(jnp.float32)
        owned.append(part)
    grad_keys_ref[...] = (owned[0] * scaling).astype(jnp.bfloat16)
    grad_values_ref[...] = owned[1].astype(jnp.bfloat16)

    for distance in range(1, REACH + 1):
        sent = direct(distance, me)
        if distance > HALF:
            sent = (me >= distance - HALF) & (me + HALF < count)

        @pl.when(sent)
        def _():
            for half in range(2):
                key_copy(distance, half).wait_send()

        @pl.when(me >= distance)
        def _():
            grad_copy(distance).wait_send()

    for fits, slot, step in turns:

        @pl.when(fits)
        def _():
            for half in range(2):
                key_copy(slot, half, step).wait_send()


def settle(*refs):
    copies = [
        pltpu.make_async_copy(refs[index], refs[4 + index], refs[8].at[index])
        for index in range(4)
    ]
    for copy in copies:
        copy.start()
    for copy in copies:
        copy.wait()


def per_device(queries, keys, values, cotangent, doc_lengths):
    rows, head_size = keys.shape
    head_count = queries.shape[1] // head_size
    members = lax.axis_size("grp")
    count = lax.axis_size("seq") * members
    tall = (REACH + 1) * rows
    wide = head_count * rows
    vmem = pl.BlockSpec(memory_space=pltpu.VMEM)
    far = pl.BlockSpec(memory_space=pltpu.HBM)
    low, full = jnp.bfloat16, jnp.float32
    operands = (doc_lengths, queries, keys, values, cotangent)
    results = pl.pallas_call(
        functools.partial(kernel, count, members),
        out_shape=tuple(
            pltpu.VMEM(part.shape, low) for part in (queries, queries, keys, keys)
        ),
        in_specs=[far] * 5,
        out_specs=(vmem,) * 4,
        scratch_shapes=[
            pltpu.VMEM((REACH + 1, 2, rows, head_size), low),
            pltpu.VMEM((head_size, wide), low),
            pltpu.VMEM((head_size, wide), low),
            pltpu.VMEM((head_size, tall), low),
            pltpu.VMEM((head_size, tall), low),
            pltpu.VMEM((tall, wide), full),
            pltpu.VMEM((tall, wide), full),
            pltpu.VMEM((REACH + 1, 8, wide), full),
            pltpu.VMEM((REACH + 1, 8, wide), full),
            pltpu.VMEM((REACH + 1, 8, wide), full),
            pltpu.VMEM((8, wide), full),
            pltpu.VMEM((tall, wide), low),
            pltpu.VMEM((tall, wide), low),
            pltpu.VMEM((2, tall, head_size), full),
            pltpu.VMEM((REACH + 1, 2, rows, head_size), low),
            pltpu.VMEM((HALF + 1, 2, rows, head_size), low),
            pltpu.VMEM((HALF + 1, 2, rows, head_size), low),
            pltpu.SemaphoreType.DMA((REACH + 1, 2)),
            pltpu.SemaphoreType.DMA((REACH + 1, 2)),
            pltpu.SemaphoreType.DMA((REACH + 1,)),
            pltpu.SemaphoreType.DMA((REACH + 1,)),
            pltpu.SMEM(doc_lengths.shape, jnp.int32),
            pltpu.VMEM((wide, 2 * head_size), low),
            pltpu.VMEM(keys.shape, low),
            pltpu.VMEM(keys.shape, low),
            pltpu.SemaphoreType.DMA((3 + 2 * head_count,)),
        ],
        compiler_params=pltpu.CompilerParams(
            collective_id=0, has_side_effects=True, vmem_limit_bytes=50000 * 1024
        ),
        name="attention",
    )(*(pltpu.with_memory_space_constraint(part, pltpu.HBM) for part in operands))
    return pl.pallas_call(
        settle,
        out_shape=tuple(jax.ShapeDtypeStruct(result.shape, low) for result in results),
        in_specs=[vmem] * 4,
        out_specs=(far,) * 4,
        scratch_shapes=[pltpu.SemaphoreType.DMA((4,))],
        compiler_params=pltpu.CompilerParams(vmem_limit_bytes=4096 * 1024),
        name="settle",
    )(*results)


def solution(mesh):
    rows = P(("seq", "grp"), None)
    return jax.shard_map(
        per_device,
        mesh=mesh,
        in_specs=(rows, rows, rows, rows, P()),
        out_specs=(rows, rows, rows, rows),
        check_vma=False,
    )
```

```python
import functools

import jax
import jax.numpy as jnp
from jax import lax
from jax.experimental import pallas as pl
from jax.experimental.pallas import tpu as pltpu
from jax.sharding import PartitionSpec as P

REACH = 8
HALF = REACH // 2
GROUP_HEADS = 4
MASKED = -1e30
LOG2E = 1.4426950408889634
PLACES = (0, 1, 3, 4, 2, 5, 6, 7, 8)


def kernel(
    count,
    members,
    lengths_hbm,
    queries_hbm,
    keys_hbm,
    values_hbm,
    cotangent_hbm,
    out_ref,
    grad_queries_ref,
    grad_keys_ref,
    grad_values_ref,
    window,
    queries_t,
    cotangent_t,
    keys_t,
    values_t,
    probs,
    grad_probs,
    peaks,
    sums,
    dots,
    row_dots,
    weights_low,
    grad_scores,
    grad_window,
    grad_send,
    grad_far,
    grad_near,
    send_sems,
    recv_sems,
    grad_send_sems,
    grad_recv_sems,
    lengths_ref,
    stacked,
    keys_ref,
    values_ref,
    load_sems,
):
    rows, head_size = keys_ref.shape
    head_count = stacked.shape[0] // rows
    heads = min(head_count, GROUP_HEADS)
    width = heads * rows
    groups = head_count // heads
    scaling = head_size ** (-0.5)
    me = lax.axis_index("seq") * members + lax.axis_index("grp")

    def place(index):
        return (lax.div(index, members), lax.rem(index, members))

    member = lax.axis_index("grp")
    paired = members == HALF

    def key_copy(distance, half, step=None):
        if step is not None:
            source, slot, sender = window.at[distance, half], distance + step, 0
        elif distance > HALF:
            source, slot, sender = window.at[distance - HALF, half], distance, distance
            step = HALF
        else:
            source, slot, sender = (keys_ref, values_ref)[half], distance, distance
            step = distance
        return pltpu.make_async_remote_copy(
            src_ref=source,
            dst_ref=window.at[slot, half],
            send_sem=send_sems.at[sender, half],
            recv_sem=recv_sems.at[slot, half],
            device_id=place(me + step),
            device_id_type=pl.DeviceIdType.MESH,
        )

    def direct(distance, sender):
        within = (sender >= 0) & (sender + distance < count)
        if paired and distance == 1:
            within = within & (lax.rem(sender + members, members) <= members - 2)
        if paired and distance == HALF - 1:
            within = within & (lax.rem(sender + members, members) >= 1)
        return within

    turns = ()
    if paired:
        middle = HALF // 2
        turns = (
            ((member == middle - 1) & (me >= middle), middle, -1),
            (member == middle, middle, 1),
        )

    def pass_on(distance, half):
        for fits, slot, step in turns:
            if slot == distance:

                @pl.when(fits)
                def _():
                    key_copy(distance, half, step).start()

        @pl.when((me >= distance) & (me + HALF < count))
        def _():
            key_copy(distance + HALF, half).start()

    def grad_copy(distance, half):
        if distance > HALF:
            target, slot = me - HALF, grad_far.at[distance - HALF, half]
        else:
            target, slot = me - distance, grad_near.at[distance, half]
        return pltpu.make_async_remote_copy(
            src_ref=grad_send.at[distance, half],
            dst_ref=slot,
            send_sem=grad_send_sems.at[distance, half],
            recv_sem=grad_recv_sems.at[distance, half],
            device_id=place(target),
            device_id_type=pl.DeviceIdType.MESH,
        )

    pairs = [
        (keys_hbm, keys_ref),
        (values_hbm, values_ref),
        (lengths_hbm, lengths_ref),
    ]
    for half, source in enumerate((queries_hbm, cotangent_hbm)):
        for head in range(head_count):
            pairs.append(
                (
                    source.at[:, head * head_size : (head + 1) * head_size],
                    stacked.at[
                        head * rows : (head + 1) * rows,
                        half * head_size : (half + 1) * head_size,
                    ],
                )
            )
    loads = [
        pltpu.make_async_copy(source, target, load_sems.at[index])
        for index, (source, target) in enumerate(pairs)
    ]
    for load in loads[:2]:
        load.start()

    barrier = pltpu.get_barrier_semaphore()
    greeted = jnp.int32(0)
    for distance in range(HALF, 0, -1):
        for fits, there in (
            (direct(distance, me), me + distance),
            (direct(distance, me - distance), me - distance),
        ):
            greeted = greeted + fits.astype(jnp.int32)

            @pl.when(fits)
            def _():
                pl.semaphore_signal(
                    barrier, inc=1, device_id=place(there), device_id_type=pl.DeviceIdType.MESH
                )

    for load in loads[2:]:
        load.start()

    for distance in range(1, REACH + 1):

        @pl.when(me < distance)
        def _():
            window[distance] = jnp.zeros_like(window.at[distance])

    for distance in range(1, HALF + 1):

        @pl.when(me + distance >= count)
        def _():
            grad_near[distance] = jnp.zeros_like(grad_near.at[distance])

        @pl.when((me + HALF >= count) | (me < distance))
        def _():
            grad_far[distance] = jnp.zeros_like(grad_far.at[distance])

    for load in loads[:3]:
        load.wait()
    query_pos = me * rows + lax.broadcasted_iota(jnp.int32, (1, rows), 1)

    def one_doc(doc, state):
        end, start = state
        end = end + lengths_ref[doc]
        return end, jnp.where(query_pos >= end, end, start)

    _, doc_start = lax.fori_loop(
        0, lengths_ref.shape[0], one_doc, (jnp.int32(0), jnp.zeros((1, rows), jnp.int32))
    )

    for load in loads[3:]:
        load.wait()
    for head in range(head_count):
        columns = slice(head * rows, (head + 1) * rows)
        queries_t[:, columns] = stacked[columns, 0:head_size].T
        cotangent_t[:, columns] = stacked[columns, head_size:].T

    def block_rows(distance):
        return slice(PLACES[distance] * rows, (PLACES[distance] + 1) * rows)

    def block_of(distance):
        if distance == 0:
            return keys_ref[...], values_ref[...]
        return window[distance, 0], window[distance, 1]

    def score_block(distance):
        keys, values = block_of(distance)
        span = block_rows(distance)
        keys_t[:, span] = keys.T
        values_t[:, span] = values.T
        key_pos = (me - distance) * rows + lax.broadcasted_iota(jnp.int32, (rows, rows), 0)
        allowed = key_pos >= doc_start
        if distance == 0:
            allowed = allowed & (key_pos <= query_pos)
        bias = jnp.where(allowed, 0.0, MASKED).astype(jnp.float32)
        bias = jnp.concatenate([bias] * heads, axis=1)

        def folded(part, op):
            return op(part.reshape(rows // 8, 8, width), axis=0)

        for group in range(groups):
            columns = slice(group * width, (group + 1) * width)
            scores = jnp.dot(keys, queries_t[:, columns], preferred_element_type=jnp.float32)
            scores = scores * (scaling * LOG2E) + bias
            peak = folded(scores, jnp.max)
            prob = jnp.exp2(scores.reshape(rows // 8, 8, width) - peak[None]).reshape(rows, width)
            grad_prob = jnp.dot(values, cotangent_t[:, columns], preferred_element_type=jnp.float32)
            probs[span, columns] = prob
            grad_probs[span, columns] = grad_prob
            peaks[distance, :, columns] = peak
            sums[distance, :, columns] = folded(prob, jnp.sum)
            dots[distance, :, columns] = folded(prob * grad_prob, jnp.sum)

    score_block(0)
    pl.semaphore_wait(barrier, greeted)
    for distance in (4, 2, 1, 3):

        @pl.when(direct(distance, me))
        def _():
            for half in range(2):
                key_copy(distance, half).start()

    for distance in (4, 2, 3, 1, 8, 6, 7, 5):
        for half in range(2):

            @pl.when(me >= distance)
            def _():
                key_copy(distance, half).wait_recv()

            if distance <= HALF:
                pass_on(distance, half)
        score_block(distance)

    for group in range(groups):
        columns = slice(group * width, (group + 1) * width)
        top = peaks[0, :, columns]
        for distance in range(1, REACH + 1):
            top = jnp.maximum(top, peaks[distance, :, columns])
        top = jnp.max(top, axis=0, keepdims=True)
        total = jnp.zeros((8, width), jnp.float32)
        dot = total
        for distance in range(REACH + 1):
            factor = jnp.exp2(peaks[distance, :, columns] - top)
            peaks[distance, :, columns] = factor
            total = total + factor * sums[distance, :, columns]
            dot = dot + factor * dots[distance, :, columns]
        inverse = 1.0 / jnp.sum(total, axis=0, keepdims=True)
        row_dots[:, columns] = jnp.broadcast_to(
            jnp.sum(dot, axis=0, keepdims=True) * inverse, (8, width)
        )
        for distance in range(REACH + 1):
            peaks[distance, :, columns] = peaks[distance, :, columns] * inverse

    def grad_block(distance):
        block = block_rows(distance)
        tiles = (rows // 8, 8, width)
        for group in range(groups):
            columns = slice(group * width, (group + 1) * width)
            weights = probs[block, columns].reshape(tiles) * peaks[distance, :, columns][None]
            weights_low[block, columns] = weights.reshape(rows, width).astype(jnp.bfloat16)
            grads = weights * (
                grad_probs[block, columns].reshape(tiles) - row_dots[:, columns][None]
            )
            grad_scores[block, columns] = grads.reshape(rows, width).astype(jnp.bfloat16)
        for half, left in enumerate((grad_scores, weights_low)):
            part = jnp.dot(left[block, :], stacked[:, half * head_size : (half + 1) * head_size], preferred_element_type=jnp.float32)
            if distance > HALF:
                grad_send[distance, half] = part.astype(jnp.bfloat16)
            else:
                grad_window[half, block, :] = part

    def send_far(distance):
        @pl.when(me >= distance)
        def _():
            for half in range(2):
                grad_copy(distance, half).start()

    def send_near(distance):
        block = block_rows(distance)
        for half in range(2):

            @pl.when((me >= distance) & (me + HALF < count))
            def _():
                grad_copy(distance + HALF, half).wait_recv()

            @pl.when(me >= distance)
            def _():
                grad_send[distance, half] = (
                    grad_window[half, block, :] + grad_far[distance, half].astype(jnp.float32)
                ).astype(jnp.bfloat16)
                grad_copy(distance, half).start()

    def finish(group):
        columns = slice(group * width, (group + 1) * width)
        out_part = jnp.dot(
            values_t[...], weights_low[:, columns], preferred_element_type=jnp.float32
        ).astype(jnp.bfloat16)
        grad_part = jnp.dot(
            keys_t[...], grad_scores[:, columns], preferred_element_type=jnp.float32
        )
        grad_part = (grad_part * scaling).astype(jnp.bfloat16)
        for head in range(heads):
            local = slice(head * rows, (head + 1) * rows)
            first = (group * heads + head) * head_size
            out_ref[:, first : first + head_size] = out_part[:, local].T
            grad_queries_ref[:, first : first + head_size] = grad_part[:, local].T

    for distance in (7, 6, 5, 8):
        grad_block(distance)
        send_far(distance)
    grad_block(3)
    grad_block(2)
    grad_block(1)
    send_near(3)
    grad_block(4)
    grad_block(0)
    send_near(2)
    pending = list(range(groups))
    early = groups // 2
    for group in pending[:early]:
        finish(group)
    send_near(1)
    for group in pending[early:]:
        finish(group)
    send_near(4)

    for distance in range(1, HALF + 1):

        @pl.when(me + distance < count)
        def _():
            for half in range(2):
                grad_copy(distance, half).wait_recv()

    owned = []
    for half in range(2):
        part = grad_window[half, 0:rows, :]
        for distance in range(1, HALF + 1):
            part = part + grad_near[distance, half].astype(jnp.float32)
        owned.append(part)
    grad_keys_ref[...] = (owned[0] * scaling).astype(jnp.bfloat16)
    grad_values_ref[...] = owned[1].astype(jnp.bfloat16)

    for distance in range(1, REACH + 1):
        sent = direct(distance, me)
        if distance > HALF:
            sent = (me >= distance - HALF) & (me + HALF < count)

        @pl.when(sent)
        def _():
            for half in range(2):
                key_copy(distance, half).wait_send()

        @pl.when(me >= distance)
        def _():
            for half in range(2):
                grad_copy(distance, half).wait_send()

    for fits, slot, step in turns:

        @pl.when(fits)
        def _():
            for half in range(2):
                key_copy(slot, half, step).wait_send()


def settle(*refs):
    copies = [
        pltpu.make_async_copy(refs[index], refs[4 + index], refs[8].at[index])
        for index in range(4)
    ]
    for copy in copies:
        copy.start()
    for copy in copies:
        copy.wait()


def per_device(queries, keys, values, cotangent, doc_lengths):
    rows, head_size = keys.shape
    head_count = queries.shape[1] // head_size
    members = lax.axis_size("grp")
    count = lax.axis_size("seq") * members
    tall = (REACH + 1) * rows
    wide = head_count * rows
    vmem = pl.BlockSpec(memory_space=pltpu.VMEM)
    far = pl.BlockSpec(memory_space=pltpu.HBM)
    low, full = jnp.bfloat16, jnp.float32
    operands = (doc_lengths, queries, keys, values, cotangent)
    results = pl.pallas_call(
        functools.partial(kernel, count, members),
        out_shape=tuple(
            pltpu.VMEM(part.shape, low) for part in (queries, queries, keys, keys)
        ),
        in_specs=[far] * 5,
        out_specs=(vmem,) * 4,
        scratch_shapes=[
            pltpu.VMEM((REACH + 1, 2, rows, head_size), low),
            pltpu.VMEM((head_size, wide), low),
            pltpu.VMEM((head_size, wide), low),
            pltpu.VMEM((head_size, tall), low),
            pltpu.VMEM((head_size, tall), low),
            pltpu.VMEM((tall, wide), full),
            pltpu.VMEM((tall, wide), full),
            pltpu.VMEM((REACH + 1, 8, wide), full),
            pltpu.VMEM((REACH + 1, 8, wide), full),
            pltpu.VMEM((REACH + 1, 8, wide), full),
            pltpu.VMEM((8, wide), full),
            pltpu.VMEM((tall, wide), low),
            pltpu.VMEM((tall, wide), low),
            pltpu.VMEM((2, tall, head_size), full),
            pltpu.VMEM((REACH + 1, 2, rows, head_size), low),
            pltpu.VMEM((HALF + 1, 2, rows, head_size), low),
            pltpu.VMEM((HALF + 1, 2, rows, head_size), low),
            pltpu.SemaphoreType.DMA((REACH + 1, 2)),
            pltpu.SemaphoreType.DMA((REACH + 1, 2)),
            pltpu.SemaphoreType.DMA((REACH + 1, 2)),
            pltpu.SemaphoreType.DMA((REACH + 1, 2)),
            pltpu.SMEM(doc_lengths.shape, jnp.int32),
            pltpu.VMEM((wide, 2 * head_size), low),
            pltpu.VMEM(keys.shape, low),
            pltpu.VMEM(keys.shape, low),
            pltpu.SemaphoreType.DMA((3 + 2 * head_count,)),
        ],
        compiler_params=pltpu.CompilerParams(
            collective_id=0, has_side_effects=True, vmem_limit_bytes=50000 * 1024
        ),
        name="attention",
    )(*(pltpu.with_memory_space_constraint(part, pltpu.HBM) for part in operands))
    return pl.pallas_call(
        settle,
        out_shape=tuple(jax.ShapeDtypeStruct(result.shape, low) for result in results),
        in_specs=[vmem] * 4,
        out_specs=(far,) * 4,
        scratch_shapes=[pltpu.SemaphoreType.DMA((4,))],
        compiler_params=pltpu.CompilerParams(vmem_limit_bytes=4096 * 1024),
        name="settle",
    )(*results)


def solution(mesh):
    rows = P(("seq", "grp"), None)
    return jax.shard_map(
        per_device,
        mesh=mesh,
        in_specs=(rows, rows, rows, rows, P()),
        out_specs=(rows, rows, rows, rows),
        check_vma=False,
    )
```

```python
import functools

import jax
import jax.numpy as jnp
from jax import lax
from jax.experimental import pallas as pl
from jax.experimental.pallas import tpu as pltpu
from jax.sharding import PartitionSpec as P

REACH = 8
HALF = REACH // 2
GROUP_HEADS = 4
MASKED = -1e30
LOG2E = 1.4426950408889634
PLACES = (0, 1, 3, 4, 2, 5, 6, 7, 8)


def kernel(
    count,
    members,
    lengths_hbm,
    queries_hbm,
    keys_hbm,
    values_hbm,
    cotangent_hbm,
    out_ref,
    grad_queries_ref,
    grad_keys_ref,
    grad_values_ref,
    window,
    queries_t,
    cotangent_t,
    keys_t,
    values_t,
    probs,
    grad_probs,
    peaks,
    sums,
    dots,
    row_dots,
    weights_low,
    grad_scores,
    grad_window,
    grad_send,
    grad_far,
    grad_near,
    send_sems,
    recv_sems,
    grad_send_sems,
    grad_recv_sems,
    lengths_ref,
    stacked,
    keys_ref,
    values_ref,
    load_sems,
):
    rows, head_size = keys_ref.shape
    head_count = stacked.shape[0] // rows
    heads = min(head_count, GROUP_HEADS)
    width = heads * rows
    groups = head_count // heads
    scaling = head_size ** (-0.5)
    me = lax.axis_index("seq") * members + lax.axis_index("grp")

    def place(index):
        return (lax.div(index, members), lax.rem(index, members))

    member = lax.axis_index("grp")
    paired = members == HALF

    def key_copy(distance, half, step=None):
        if step is not None:
            source, slot, sender = window.at[distance, half], distance + step, 0
        elif distance > HALF:
            source, slot, sender = window.at[distance - HALF, half], distance, distance
            step = HALF
        else:
            source, slot, sender = (keys_ref, values_ref)[half], distance, distance
            step = distance
        return pltpu.make_async_remote_copy(
            src_ref=source,
            dst_ref=window.at[slot, half],
            send_sem=send_sems.at[sender, half],
            recv_sem=recv_sems.at[slot, half],
            device_id=place(me + step),
            device_id_type=pl.DeviceIdType.MESH,
        )

    def direct(distance, sender):
        within = (sender >= 0) & (sender + distance < count)
        if paired and distance == 1:
            within = within & (lax.rem(sender + members, members) <= members - 2)
        if paired and distance == HALF - 1:
            within = within & (lax.rem(sender + members, members) >= 1)
        return within

    turns = ()
    if paired:
        middle = HALF // 2
        turns = (
            ((member == middle - 1) & (me >= middle), middle, -1),
            (member == middle, middle, 1),
        )

    def pass_on(distance, half):
        for fits, slot, step in turns:
            if slot == distance:

                @pl.when(fits)
                def _():
                    key_copy(distance, half, step).start()

        @pl.when((me >= distance) & (me + HALF < count))
        def _():
            key_copy(distance + HALF, half).start()

    def grad_copy(distance, half):
        if distance > HALF:
            target, slot = me - HALF, grad_far.at[distance - HALF, half]
        else:
            target, slot = me - distance, grad_near.at[distance, half]
        return pltpu.make_async_remote_copy(
            src_ref=grad_send.at[distance, half],
            dst_ref=slot,
            send_sem=grad_send_sems.at[distance, half],
            recv_sem=grad_recv_sems.at[distance, half],
            device_id=place(target),
            device_id_type=pl.DeviceIdType.MESH,
        )

    pairs = [
        (keys_hbm, keys_ref),
        (values_hbm, values_ref),
        (lengths_hbm, lengths_ref),
    ]
    for half, source in enumerate((queries_hbm, cotangent_hbm)):
        for head in range(head_count):
            pairs.append(
                (
                    source.at[:, head * head_size : (head + 1) * head_size],
                    stacked.at[
                        head * rows : (head + 1) * rows,
                        half * head_size : (half + 1) * head_size,
                    ],
                )
            )
    loads = [
        pltpu.make_async_copy(source, target, load_sems.at[index])
        for index, (source, target) in enumerate(pairs)
    ]
    for load in loads[:2]:
        load.start()

    barrier = pltpu.get_barrier_semaphore()
    greeted = jnp.int32(0)
    for distance in range(HALF, 0, -1):
        for fits, there in (
            (direct(distance, me), me + distance),
            (direct(distance, me - distance), me - distance),
        ):
            greeted = greeted + fits.astype(jnp.int32)

            @pl.when(fits)
            def _():
                pl.semaphore_signal(
                    barrier, inc=1, device_id=place(there), device_id_type=pl.DeviceIdType.MESH
                )

    for load in loads[2:]:
        load.start()

    for distance in range(1, REACH + 1):

        @pl.when(me < distance)
        def _():
            window[distance] = jnp.zeros_like(window.at[distance])

    for distance in range(1, HALF + 1):

        @pl.when(me + distance >= count)
        def _():
            grad_near[distance] = jnp.zeros_like(grad_near.at[distance])

        @pl.when((me + HALF >= count) | (me < distance))
        def _():
            grad_far[distance] = jnp.zeros_like(grad_far.at[distance])

    for load in loads[:3]:
        load.wait()
    query_pos = me * rows + lax.broadcasted_iota(jnp.int32, (1, rows), 1)

    def one_doc(doc, state):
        end, start = state
        end = end + lengths_ref[doc]
        return end, jnp.where(query_pos >= end, end, start)

    _, doc_start = lax.fori_loop(
        0, lengths_ref.shape[0], one_doc, (jnp.int32(0), jnp.zeros((1, rows), jnp.int32))
    )

    for load in loads[3:]:
        load.wait()
    for head in range(head_count):
        columns = slice(head * rows, (head + 1) * rows)
        queries_t[:, columns] = stacked[columns, 0:head_size].T
        cotangent_t[:, columns] = stacked[columns, head_size:].T

    def block_rows(distance):
        return slice(PLACES[distance] * rows, (PLACES[distance] + 1) * rows)

    def block_of(distance):
        if distance == 0:
            return keys_ref[...], values_ref[...]
        return window[distance, 0], window[distance, 1]

    def score_block(distance):
        keys, values = block_of(distance)
        span = block_rows(distance)
        keys_t[:, span] = keys.T
        values_t[:, span] = values.T
        key_pos = (me - distance) * rows + lax.broadcasted_iota(jnp.int32, (rows, rows), 0)
        allowed = key_pos >= doc_start
        if distance == 0:
            allowed = allowed & (key_pos <= query_pos)
        bias = jnp.where(allowed, 0.0, MASKED).astype(jnp.float32)
        bias = jnp.concatenate([bias] * heads, axis=1)

        def folded(part, op):
            return op(part.reshape(rows // 8, 8, width), axis=0)

        for group in range(groups):
            columns = slice(group * width, (group + 1) * width)
            scores = jnp.dot(keys, queries_t[:, columns], preferred_element_type=jnp.float32)
            scores = scores * (scaling * LOG2E) + bias
            peak = folded(scores, jnp.max)
            prob = jnp.exp2(scores.reshape(rows // 8, 8, width) - peak[None]).reshape(rows, width)
            grad_prob = jnp.dot(values, cotangent_t[:, columns], preferred_element_type=jnp.float32)
            probs[span, columns] = prob
            grad_probs[span, columns] = grad_prob
            peaks[distance, :, columns] = peak
            sums[distance, :, columns] = folded(prob, jnp.sum)
            dots[distance, :, columns] = folded(prob * grad_prob, jnp.sum)

    score_block(0)
    pl.semaphore_wait(barrier, greeted)
    for distance in (4, 2, 1, 3):

        @pl.when(direct(distance, me))
        def _():
            for half in range(2):
                key_copy(distance, half).start()

    for distance in (4, 2, 3, 1, 8, 6, 7, 5):
        for half in range(2):

            @pl.when(me >= distance)
            def _():
                key_copy(distance, half).wait_recv()

            if distance <= HALF:
                pass_on(distance, half)
        score_block(distance)

    for group in range(groups):
        columns = slice(group * width, (group + 1) * width)
        top = peaks[0, :, columns]
        for distance in range(1, REACH + 1):
            top = jnp.maximum(top, peaks[distance, :, columns])
        top = jnp.max(top, axis=0, keepdims=True)
        total = jnp.zeros((8, width), jnp.float32)
        dot = total
        for distance in range(REACH + 1):
            factor = jnp.exp2(peaks[distance, :, columns] - top)
            peaks[distance, :, columns] = factor
            total = total + factor * sums[distance, :, columns]
            dot = dot + factor * dots[distance, :, columns]
        inverse = 1.0 / jnp.sum(total, axis=0, keepdims=True)
        row_dots[:, columns] = jnp.broadcast_to(
            jnp.sum(dot, axis=0, keepdims=True) * inverse, (8, width)
        )
        for distance in range(REACH + 1):
            peaks[distance, :, columns] = peaks[distance, :, columns] * inverse

    def grad_blocks(*distances):
        first = min(PLACES[distance] for distance in distances)
        span = slice(first * rows, (first + len(distances)) * rows)
        tiles = (rows // 8, 8, width)
        for group in range(groups):
            columns = slice(group * width, (group + 1) * width)
            for distance in distances:
                block = block_rows(distance)
                factor = peaks[distance, :, columns][None]
                weights = probs[block, columns].reshape(tiles) * factor
                weights_low[block, columns] = weights.reshape(rows, width).astype(jnp.bfloat16)
                grads = weights * (
                    grad_probs[block, columns].reshape(tiles) - row_dots[:, columns][None]
                )
                grad_scores[block, columns] = grads.reshape(rows, width).astype(jnp.bfloat16)
        for half, left in enumerate((grad_scores, weights_low)):
            part = jnp.dot(left[span, :], stacked[...], preferred_element_type=jnp.float32)
            part = part[:, half * head_size : (half + 1) * head_size]
            for distance in distances:
                local = (PLACES[distance] - first) * rows
                piece = part[local : local + rows, :]
                if distance > HALF:
                    grad_send[distance, half] = piece.astype(jnp.bfloat16)
                else:
                    grad_window[half, block_rows(distance), :] = piece

    def send_far(distance):
        @pl.when(me >= distance)
        def _():
            for half in range(2):
                grad_copy(distance, half).start()

    def send_near(distance):
        block = block_rows(distance)
        for half in range(2):

            @pl.when((me >= distance) & (me + HALF < count))
            def _():
                grad_copy(distance + HALF, half).wait_recv()

            @pl.when(me >= distance)
            def _():
                grad_send[distance, half] = (
                    grad_window[half, block, :] + grad_far[distance, half].astype(jnp.float32)
                ).astype(jnp.bfloat16)
                grad_copy(distance, half).start()

    def finish(group):
        columns = slice(group * width, (group + 1) * width)
        out_part = jnp.dot(
            values_t[...], weights_low[:, columns], preferred_element_type=jnp.float32
        ).astype(jnp.bfloat16)
        grad_part = jnp.dot(
            keys_t[...], grad_scores[:, columns], preferred_element_type=jnp.float32
        )
        grad_part = (grad_part * scaling).astype(jnp.bfloat16)
        for head in range(heads):
            local = slice(head * rows, (head + 1) * rows)
            first = (group * heads + head) * head_size
            out_ref[:, first : first + head_size] = out_part[:, local].T
            grad_queries_ref[:, first : first + head_size] = grad_part[:, local].T

    grad_blocks(6, 7)
    send_far(7)
    send_far(6)
    grad_blocks(5)
    send_far(5)
    grad_blocks(8)
    send_far(8)
    grad_blocks(2, 3)
    send_near(3)
    send_near(2)
    grad_blocks(1, 4)
    send_near(1)
    send_near(4)
    grad_blocks(0)
    finish(0)
    finish(1)
    finish(2)
    finish(3)

    for distance in range(1, HALF + 1):

        @pl.when(me + distance < count)
        def _():
            for half in range(2):
                grad_copy(distance, half).wait_recv()

    owned = []
    for half in range(2):
        part = grad_window[half, 0:rows, :]
        for distance in range(1, HALF + 1):
            part = part + grad_near[distance, half].astype(jnp.float32)
        owned.append(part)
    grad_keys_ref[...] = (owned[0] * scaling).astype(jnp.bfloat16)
    grad_values_ref[...] = owned[1].astype(jnp.bfloat16)

    for distance in range(1, REACH + 1):
        sent = direct(distance, me)
        if distance > HALF:
            sent = (me >= distance - HALF) & (me + HALF < count)

        @pl.when(sent)
        def _():
            for half in range(2):
                key_copy(distance, half).wait_send()

        @pl.when(me >= distance)
        def _():
            for half in range(2):
                grad_copy(distance, half).wait_send()

    for fits, slot, step in turns:

        @pl.when(fits)
        def _():
            for half in range(2):
                key_copy(slot, half, step).wait_send()


def settle(*refs):
    copies = [
        pltpu.make_async_copy(refs[index], refs[4 + index], refs[8].at[index])
        for index in range(4)
    ]
    for copy in copies:
        copy.start()
    for copy in copies:
        copy.wait()


def per_device(queries, keys, values, cotangent, doc_lengths):
    rows, head_size = keys.shape
    head_count = queries.shape[1] // head_size
    members = lax.axis_size("grp")
    count = lax.axis_size("seq") * members
    tall = (REACH + 1) * rows
    wide = head_count * rows
    vmem = pl.BlockSpec(memory_space=pltpu.VMEM)
    far = pl.BlockSpec(memory_space=pltpu.HBM)
    low, full = jnp.bfloat16, jnp.float32
    operands = (doc_lengths, queries, keys, values, cotangent)
    results = pl.pallas_call(
        functools.partial(kernel, count, members),
        out_shape=tuple(
            pltpu.VMEM(part.shape, low) for part in (queries, queries, keys, keys)
        ),
        in_specs=[far] * 5,
        out_specs=(vmem,) * 4,
        scratch_shapes=[
            pltpu.VMEM((REACH + 1, 2, rows, head_size), low),
            pltpu.VMEM((head_size, wide), low),
            pltpu.VMEM((head_size, wide), low),
            pltpu.VMEM((head_size, tall), low),
            pltpu.VMEM((head_size, tall), low),
            pltpu.VMEM((tall, wide), full),
            pltpu.VMEM((tall, wide), full),
            pltpu.VMEM((REACH + 1, 8, wide), full),
            pltpu.VMEM((REACH + 1, 8, wide), full),
            pltpu.VMEM((REACH + 1, 8, wide), full),
            pltpu.VMEM((8, wide), full),
            pltpu.VMEM((tall, wide), low),
            pltpu.VMEM((tall, wide), low),
            pltpu.VMEM((2, tall, head_size), full),
            pltpu.VMEM((REACH + 1, 2, rows, head_size), low),
            pltpu.VMEM((HALF + 1, 2, rows, head_size), low),
            pltpu.VMEM((HALF + 1, 2, rows, head_size), low),
            pltpu.SemaphoreType.DMA((REACH + 1, 2)),
            pltpu.SemaphoreType.DMA((REACH + 1, 2)),
            pltpu.SemaphoreType.DMA((REACH + 1, 2)),
            pltpu.SemaphoreType.DMA((REACH + 1, 2)),
            pltpu.SMEM(doc_lengths.shape, jnp.int32),
            pltpu.VMEM((wide, 2 * head_size), low),
            pltpu.VMEM(keys.shape, low),
            pltpu.VMEM(keys.shape, low),
            pltpu.SemaphoreType.DMA((3 + 2 * head_count,)),
        ],
        compiler_params=pltpu.CompilerParams(
            collective_id=0, has_side_effects=True, vmem_limit_bytes=50000 * 1024
        ),
        name="attention",
    )(*(pltpu.with_memory_space_constraint(part, pltpu.HBM) for part in operands))
    return pl.pallas_call(
        settle,
        out_shape=tuple(jax.ShapeDtypeStruct(result.shape, low) for result in results),
        in_specs=[vmem] * 4,
        out_specs=(far,) * 4,
        scratch_shapes=[pltpu.SemaphoreType.DMA((4,))],
        compiler_params=pltpu.CompilerParams(vmem_limit_bytes=4096 * 1024),
        name="settle",
    )(*results)


def solution(mesh):
    rows = P(("seq", "grp"), None)
    return jax.shard_map(
        per_device,
        mesh=mesh,
        in_specs=(rows, rows, rows, rows, P()),
        out_specs=(rows, rows, rows, rows),
        check_vma=False,
    )
```

```python
import functools

import jax
import jax.numpy as jnp
from jax import lax
from jax.experimental import pallas as pl
from jax.experimental.pallas import tpu as pltpu
from jax.sharding import PartitionSpec as P

REACH = 8
HALF = REACH // 2
GROUP_HEADS = 8
MASKED = -1e30
LOG2E = 1.4426950408889634
PLACES = (0, 1, 3, 4, 2, 5, 6, 7, 8)


def kernel(
    count,
    members,
    lengths_hbm,
    queries_hbm,
    keys_hbm,
    values_hbm,
    cotangent_hbm,
    out_ref,
    grad_queries_ref,
    grad_keys_ref,
    grad_values_ref,
    window,
    queries_t,
    cotangent_t,
    keys_t,
    values_t,
    probs,
    grad_probs,
    peaks,
    sums,
    dots,
    row_dots,
    weights_low,
    grad_scores,
    grad_window,
    grad_send,
    grad_far,
    grad_near,
    send_sems,
    recv_sems,
    grad_send_sems,
    grad_recv_sems,
    lengths_ref,
    stacked,
    keys_ref,
    values_ref,
    load_sems,
):
    rows, head_size = keys_ref.shape
    head_count = stacked.shape[0] // rows
    heads = min(head_count, GROUP_HEADS)
    width = heads * rows
    groups = head_count // heads
    scaling = head_size ** (-0.5)
    me = lax.axis_index("seq") * members + lax.axis_index("grp")

    def place(index):
        return (lax.div(index, members), lax.rem(index, members))

    member = lax.axis_index("grp")
    paired = members == HALF

    def key_copy(distance, half, step=None):
        if step is not None:
            source, slot, sender = window.at[distance, half], distance + step, 0
        elif distance > HALF:
            source, slot, sender = window.at[distance - HALF, half], distance, distance
            step = HALF
        else:
            source, slot, sender = (keys_ref, values_ref)[half], distance, distance
            step = distance
        return pltpu.make_async_remote_copy(
            src_ref=source,
            dst_ref=window.at[slot, half],
            send_sem=send_sems.at[sender, half],
            recv_sem=recv_sems.at[slot, half],
            device_id=place(me + step),
            device_id_type=pl.DeviceIdType.MESH,
        )

    def direct(distance, sender):
        within = (sender >= 0) & (sender + distance < count)
        if paired and distance == 1:
            within = within & (lax.rem(sender + members, members) <= members - 2)
        if paired and distance == HALF - 1:
            within = within & (lax.rem(sender + members, members) >= 1)
        return within

    turns = ()
    if paired:
        middle = HALF // 2
        turns = (
            ((member == middle - 1) & (me >= middle), middle, -1),
            (member == middle, middle, 1),
        )

    def pass_on(distance, half):
        for fits, slot, step in turns:
            if slot == distance:

                @pl.when(fits)
                def _():
                    key_copy(distance, half, step).start()

        @pl.when((me >= distance) & (me + HALF < count))
        def _():
            key_copy(distance + HALF, half).start()

    def grad_copy(distance, half):
        if distance > HALF:
            target, slot = me - HALF, grad_far.at[distance - HALF, half]
        else:
            target, slot = me - distance, grad_near.at[distance, half]
        return pltpu.make_async_remote_copy(
            src_ref=grad_send.at[distance, half],
            dst_ref=slot,
            send_sem=grad_send_sems.at[distance, half],
            recv_sem=grad_recv_sems.at[distance, half],
            device_id=place(target),
            device_id_type=pl.DeviceIdType.MESH,
        )

    pairs = [
        (keys_hbm, keys_ref),
        (values_hbm, values_ref),
        (lengths_hbm, lengths_ref),
    ]
    for half, source in enumerate((queries_hbm, cotangent_hbm)):
        for head in range(head_count):
            pairs.append(
                (
                    source.at[:, head * head_size : (head + 1) * head_size],
                    stacked.at[
                        head * rows : (head + 1) * rows,
                        half * head_size : (half + 1) * head_size,
                    ],
                )
            )
    loads = [
        pltpu.make_async_copy(source, target, load_sems.at[index])
        for index, (source, target) in enumerate(pairs)
    ]
    for load in loads[:2]:
        load.start()

    barrier = pltpu.get_barrier_semaphore()
    greeted = jnp.int32(0)
    for distance in range(HALF, 0, -1):
        for fits, there in (
            (direct(distance, me), me + distance),
            (direct(distance, me - distance), me - distance),
        ):
            greeted = greeted + fits.astype(jnp.int32)

            @pl.when(fits)
            def _():
                pl.semaphore_signal(
                    barrier, inc=1, device_id=place(there), device_id_type=pl.DeviceIdType.MESH
                )

    for load in loads[2:]:
        load.start()

    for distance in range(1, REACH + 1):

        @pl.when(me < distance)
        def _():
            window[distance] = jnp.zeros_like(window.at[distance])

    for distance in range(1, HALF + 1):

        @pl.when(me + distance >= count)
        def _():
            grad_near[distance] = jnp.zeros_like(grad_near.at[distance])

        @pl.when((me + HALF >= count) | (me < distance))
        def _():
            grad_far[distance] = jnp.zeros_like(grad_far.at[distance])

    for load in loads[:3]:
        load.wait()
    query_pos = me * rows + lax.broadcasted_iota(jnp.int32, (1, rows), 1)

    def one_doc(doc, state):
        end, start = state
        end = end + lengths_ref[doc]
        return end, jnp.where(query_pos >= end, end, start)

    _, doc_start = lax.fori_loop(
        0, lengths_ref.shape[0], one_doc, (jnp.int32(0), jnp.zeros((1, rows), jnp.int32))
    )

    for load in loads[3:]:
        load.wait()
    for head in range(head_count):
        columns = slice(head * rows, (head + 1) * rows)
        queries_t[:, columns] = stacked[columns, 0:head_size].T
        cotangent_t[:, columns] = stacked[columns, head_size:].T

    def block_rows(distance):
        return slice(PLACES[distance] * rows, (PLACES[distance] + 1) * rows)

    def block_of(distance):
        if distance == 0:
            return keys_ref[...], values_ref[...]
        return window[distance, 0], window[distance, 1]

    def score_block(distance):
        keys, values = block_of(distance)
        span = block_rows(distance)
        keys_t[:, span] = keys.T
        values_t[:, span] = values.T
        key_pos = (me - distance) * rows + lax.broadcasted_iota(jnp.int32, (rows, rows), 0)
        allowed = key_pos >= doc_start
        if distance == 0:
            allowed = allowed & (key_pos <= query_pos)
        bias = jnp.where(allowed, 0.0, MASKED).astype(jnp.float32)
        bias = jnp.concatenate([bias] * heads, axis=1)

        def folded(part, op):
            return op(part.reshape(rows // 8, 8, width), axis=0)

        for group in range(groups):
            columns = slice(group * width, (group + 1) * width)
            scores = jnp.dot(keys, queries_t[:, columns], preferred_element_type=jnp.float32)
            scores = scores * (scaling * LOG2E) + bias
            peak = folded(scores, jnp.max)
            prob = jnp.exp2(scores.reshape(rows // 8, 8, width) - peak[None]).reshape(rows, width)
            grad_prob = jnp.dot(values, cotangent_t[:, columns], preferred_element_type=jnp.float32)
            probs[span, columns] = prob
            grad_probs[span, columns] = grad_prob
            peaks[distance, :, columns] = peak
            sums[distance, :, columns] = folded(prob, jnp.sum)
            dots[distance, :, columns] = folded(prob * grad_prob, jnp.sum)

    score_block(0)
    pl.semaphore_wait(barrier, greeted)
    for distance in (4, 2, 1, 3):

        @pl.when(direct(distance, me))
        def _():
            for half in range(2):
                key_copy(distance, half).start()

    for distance in (4, 2, 3, 1, 8, 6, 7, 5):
        for half in range(2):

            @pl.when(me >= distance)
            def _():
                key_copy(distance, half).wait_recv()

            if distance <= HALF:
                pass_on(distance, half)
        score_block(distance)

    for group in range(groups):
        columns = slice(group * width, (group + 1) * width)
        top = peaks[0, :, columns]
        for distance in range(1, REACH + 1):
            top = jnp.maximum(top, peaks[distance, :, columns])
        top = jnp.max(top, axis=0, keepdims=True)
        total = jnp.zeros((8, width), jnp.float32)
        dot = total
        for distance in range(REACH + 1):
            factor = jnp.exp2(peaks[distance, :, columns] - top)
            peaks[distance, :, columns] = factor
            total = total + factor * sums[distance, :, columns]
            dot = dot + factor * dots[distance, :, columns]
        inverse = 1.0 / jnp.sum(total, axis=0, keepdims=True)
        row_dots[:, columns] = jnp.broadcast_to(
            jnp.sum(dot, axis=0, keepdims=True) * inverse, (8, width)
        )
        for distance in range(REACH + 1):
            peaks[distance, :, columns] = peaks[distance, :, columns] * inverse

    def grad_blocks(*distances):
        first = min(PLACES[distance] for distance in distances)
        span = slice(first * rows, (first + len(distances)) * rows)
        tiles = (rows // 8, 8, width)
        for group in range(groups):
            columns = slice(group * width, (group + 1) * width)
            for distance in distances:
                block = block_rows(distance)
                factor = peaks[distance, :, columns][None]
                weights = probs[block, columns].reshape(tiles) * factor
                weights_low[block, columns] = weights.reshape(rows, width).astype(jnp.bfloat16)
                grads = weights * (
                    grad_probs[block, columns].reshape(tiles) - row_dots[:, columns][None]
                )
                grad_scores[block, columns] = grads.reshape(rows, width).astype(jnp.bfloat16)
        for half, left in enumerate((grad_scores, weights_low)):
            part = jnp.dot(left[span, :], stacked[...], preferred_element_type=jnp.float32)
            part = part[:, half * head_size : (half + 1) * head_size]
            for distance in distances:
                local = (PLACES[distance] - first) * rows
                piece = part[local : local + rows, :]
                if distance > HALF:
                    grad_send[distance, half] = piece.astype(jnp.bfloat16)
                else:
                    grad_window[half, block_rows(distance), :] = piece

    def send_far(distance):
        @pl.when(me >= distance)
        def _():
            for half in range(2):
                grad_copy(distance, half).start()

    def send_near(distance):
        block = block_rows(distance)
        for half in range(2):

            @pl.when((me >= distance) & (me + HALF < count))
            def _():
                grad_copy(distance + HALF, half).wait_recv()

            @pl.when(me >= distance)
            def _():
                grad_send[distance, half] = (
                    grad_window[half, block, :] + grad_far[distance, half].astype(jnp.float32)
                ).astype(jnp.bfloat16)
                grad_copy(distance, half).start()

    def finish(group):
        columns = slice(group * width, (group + 1) * width)
        out_part = jnp.dot(
            values_t[...], weights_low[:, columns], preferred_element_type=jnp.float32
        ).astype(jnp.bfloat16)
        grad_part = jnp.dot(
            keys_t[...], grad_scores[:, columns], preferred_element_type=jnp.float32
        )
        grad_part = (grad_part * scaling).astype(jnp.bfloat16)
        for head in range(heads):
            local = slice(head * rows, (head + 1) * rows)
            first = (group * heads + head) * head_size
            out_ref[:, first : first + head_size] = out_part[:, local].T
            grad_queries_ref[:, first : first + head_size] = grad_part[:, local].T

    grad_blocks(7, 8)
    send_far(7)
    send_far(8)
    grad_blocks(5, 6)
    send_far(6)
    send_far(5)
    grad_blocks(2, 3)
    send_near(3)
    send_near(2)
    grad_blocks(1, 4)
    send_near(1)
    grad_blocks(0)
    finish(0)
    send_near(4)
    finish(1)

    for distance in range(1, HALF + 1):

        @pl.when(me + distance < count)
        def _():
            for half in range(2):
                grad_copy(distance, half).wait_recv()

    owned = []
    for half in range(2):
        part = grad_window[half, 0:rows, :]
        for distance in range(1, HALF + 1):
            part = part + grad_near[distance, half].astype(jnp.float32)
        owned.append(part)
    grad_keys_ref[...] = (owned[0] * scaling).astype(jnp.bfloat16)
    grad_values_ref[...] = owned[1].astype(jnp.bfloat16)

    for distance in range(1, REACH + 1):
        sent = direct(distance, me)
        if distance > HALF:
            sent = (me >= distance - HALF) & (me + HALF < count)

        @pl.when(sent)
        def _():
            for half in range(2):
                key_copy(distance, half).wait_send()

        @pl.when(me >= distance)
        def _():
            for half in range(2):
                grad_copy(distance, half).wait_send()

    for fits, slot, step in turns:

        @pl.when(fits)
        def _():
            for half in range(2):
                key_copy(slot, half, step).wait_send()


def settle(*refs):
    copies = [
        pltpu.make_async_copy(refs[index], refs[4 + index], refs[8].at[index])
        for index in range(4)
    ]
    for copy in copies:
        copy.start()
    for copy in copies:
        copy.wait()


def per_device(queries, keys, values, cotangent, doc_lengths):
    rows, head_size = keys.shape
    head_count = queries.shape[1] // head_size
    members = lax.axis_size("grp")
    count = lax.axis_size("seq") * members
    tall = (REACH + 1) * rows
    wide = head_count * rows
    vmem = pl.BlockSpec(memory_space=pltpu.VMEM)
    far = pl.BlockSpec(memory_space=pltpu.HBM)
    low, full = jnp.bfloat16, jnp.float32
    operands = (doc_lengths, queries, keys, values, cotangent)
    results = pl.pallas_call(
        functools.partial(kernel, count, members),
        out_shape=tuple(
            pltpu.VMEM(part.shape, low) for part in (queries, queries, keys, keys)
        ),
        in_specs=[far] * 5,
        out_specs=(vmem,) * 4,
        scratch_shapes=[
            pltpu.VMEM((REACH + 1, 2, rows, head_size), low),
            pltpu.VMEM((head_size, wide), low),
            pltpu.VMEM((head_size, wide), low),
            pltpu.VMEM((head_size, tall), low),
            pltpu.VMEM((head_size, tall), low),
            pltpu.VMEM((tall, wide), full),
            pltpu.VMEM((tall, wide), full),
            pltpu.VMEM((REACH + 1, 8, wide), full),
            pltpu.VMEM((REACH + 1, 8, wide), full),
            pltpu.VMEM((REACH + 1, 8, wide), full),
            pltpu.VMEM((8, wide), full),
            pltpu.VMEM((tall, wide), low),
            pltpu.VMEM((tall, wide), low),
            pltpu.VMEM((2, tall, head_size), full),
            pltpu.VMEM((REACH + 1, 2, rows, head_size), low),
            pltpu.VMEM((HALF + 1, 2, rows, head_size), low),
            pltpu.VMEM((HALF + 1, 2, rows, head_size), low),
            pltpu.SemaphoreType.DMA((REACH + 1, 2)),
            pltpu.SemaphoreType.DMA((REACH + 1, 2)),
            pltpu.SemaphoreType.DMA((REACH + 1, 2)),
            pltpu.SemaphoreType.DMA((REACH + 1, 2)),
            pltpu.SMEM(doc_lengths.shape, jnp.int32),
            pltpu.VMEM((wide, 2 * head_size), low),
            pltpu.VMEM(keys.shape, low),
            pltpu.VMEM(keys.shape, low),
            pltpu.SemaphoreType.DMA((3 + 2 * head_count,)),
        ],
        compiler_params=pltpu.CompilerParams(
            collective_id=0, has_side_effects=True, vmem_limit_bytes=50000 * 1024
        ),
        name="attention",
    )(*(pltpu.with_memory_space_constraint(part, pltpu.HBM) for part in operands))
    return pl.pallas_call(
        settle,
        out_shape=tuple(jax.ShapeDtypeStruct(result.shape, low) for result in results),
        in_specs=[vmem] * 4,
        out_specs=(far,) * 4,
        scratch_shapes=[pltpu.SemaphoreType.DMA((4,))],
        compiler_params=pltpu.CompilerParams(vmem_limit_bytes=4096 * 1024),
        name="settle",
    )(*results)


def solution(mesh):
    rows = P(("seq", "grp"), None)
    return jax.shard_map(
        per_device,
        mesh=mesh,
        in_specs=(rows, rows, rows, rows, P()),
        out_specs=(rows, rows, rows, rows),
        check_vma=False,
    )
```
